32 devices in a mesh: tok: 4 (over y, x), col: 8 (over z, core).
Axes of the slice: x: 2, y: 2, z: 4, core: 2. Of those that a mesh axis runs over, the one named last changes fastest.
Arguments:
- row_bank: bfloat16 [16384, 8192], P(None, 'col'), may hold values from -50 to 50
- token_ids: int32 [6144], P('tok'), may hold values from 0 to 16383
- sign_flips: int32 [8192], P('col'), may hold values from -1 to 1, as said below
- damping: float32 [1], replicated, may hold values from 0.1 to 1
Outputs:
- hessian: float32 [8192, 8192], P('tok', 'col')
The draws below stay inside these ranges and needn't reach their ends.
Inputs may be any that keep to these rules, and one draw needn't show every extreme that they name: `sign_flips`: each entry is -1 or 1.
All inputs are finite; a program needn't handle non-finite values.
Results may differ from the reference program's by a relative error of at most 0.0003.
The reference program's roundings to bfloat16 on the way (of `picked`, `half_turned` and `rotated`) count: a program that leaves them out, or rounds other values in their place, can miss the bound.
Values may be sent and summed in bfloat16 or wider, within the bound.
A program may use at most 192 MiB of HBM per device.

```python
import math
import jax
import jax.numpy as jnp

D = 8192
BLOCK = 32
TOKENS = 6144
BANK = 16384


def draw_sign_flips(key, part):
    return 2 * jax.random.randint(key, (D,), 0, 2, dtype=jnp.int32) - 1


def draw_token_ids(key, part):
    spot = jnp.arange(TOKENS, dtype=jnp.int32)
    start = spot * (BANK // 2) // TOKENS
    jitter = jax.random.randint(jax.random.fold_in(key, 11), (TOKENS,), 0, BANK // 2, dtype=jnp.int32)
    return start + jitter


def draw_row_bank(key, part):
    place = jnp.arange(BANK, dtype=jnp.float32) / BANK
    lift = jax.random.uniform(jax.random.fold_in(key, 21), (BANK,), jnp.float32)
    row_scale = jnp.power(10.0, 0.8 * place + 0.4 * lift)
    col_scale = jnp.exp(jax.random.uniform(jax.random.fold_in(key, 22), (D,), jnp.float32) * math.log(10.0))
    noise = jnp.clip(jax.random.normal(jax.random.fold_in(key, 23), (BANK, D), jnp.float32), -6.0, 6.0)
    values = noise * row_scale[:, None] * col_scale[None, :] / 30.0
    return values.astype(jnp.bfloat16)


def setup_inputs(seed: int = 0) -> dict:
    key_list = jax.random.split(jax.random.key(seed), 5)
    row_bank = draw_row_bank(jax.random.fold_in(key_list[4], 71), 0)
    token_ids = draw_token_ids(jax.random.fold_in(key_list[4], 71), 0)
    sign_flips = draw_sign_flips(jax.random.fold_in(key_list[4], 71), 0)
    damping = jnp.clip(jnp.exp(jax.random.uniform(key_list[3], (1,), jnp.float32, math.log(0.1), math.log(1.0))), 0.1, 1.0)
    return dict(row_bank=row_bank, token_ids=token_ids, sign_flips=sign_flips, damping=damping)


def hadamard(order):
    index_range = jnp.arange(order, dtype=jnp.int32)
    anded = jnp.bitwise_and(index_range[:, None], index_range[None, :])
    parity = jnp.zeros((order, order), jnp.int32)
    for bit_place in range(int(order).bit_length()):
        parity = parity + jnp.bitwise_and(jnp.right_shift(anded, bit_place), 1)
    return (1 - 2 * jnp.bitwise_and(parity, 1)).astype(jnp.float32)

def reference(row_bank, token_ids, sign_flips, damping):
    groups = D // BLOCK
    picked = row_bank[token_ids] * sign_flips.astype(jnp.bfloat16)[None, :]
    grouped_rows = picked.reshape(TOKENS, groups, BLOCK).astype(jnp.float32)
    half_turned = jnp.einsum('rab,bc->rac', grouped_rows, hadamard(BLOCK)).astype(jnp.bfloat16)
    turned = jnp.einsum('rab,ac->rcb', half_turned.astype(jnp.float32), hadamard(groups)) * (1.0 / math.sqrt(D))
    rotated = turned.astype(jnp.bfloat16).reshape(TOKENS, D)
    gram_matrix = jnp.dot(rotated.T, rotated, preferred_element_type=jnp.float32) / TOKENS
    mean_diag = jnp.mean(jnp.diagonal(gram_matrix))
    return gram_matrix + damping[0] * mean_diag * jnp.eye(D, dtype=jnp.float32)
```

```python
import functools
import math

import jax
import jax.numpy as jnp
from jax import lax
from jax.experimental import pallas as pl
from jax.experimental.pallas import tpu as pltpu
from jax.sharding import PartitionSpec as P

D = 8192
BLOCK = 32
LANES = 512
MESH = pl.DeviceIdType.MESH


def hadamard(order):
    index_range = jnp.arange(order, dtype=jnp.int32)
    anded = jnp.bitwise_and(index_range[:, None], index_range[None, :])
    parity = jnp.zeros((order, order), jnp.int32)
    for bit_place in range(int(order).bit_length()):
        parity = parity + jnp.bitwise_and(jnp.right_shift(anded, bit_place), 1)
    return (1 - 2 * jnp.bitwise_and(parity, 1)).astype(jnp.bfloat16)


def fused_kernel(
    planes, chunks, rows, piece, scale,
    half_ref, table_ref,
    gram_ref, gram_in_ref, square_ref, full_ref,
    xbuf, tmp, rot, rxr, rxq, acc, squares,
    part_send, part_recv, z_send, z_recv, r_send, r_recv, q_send, q_recv,
    s_send, s_recv, g_send, g_recv, load_sem, out_sem,
):
    tok = lax.axis_index("tok")
    col = lax.axis_index("col")
    plane, core = col // 2, col % 2
    mate = plane * 2 + (1 - core)
    ypos, xpos = tok // 2, tok % 2
    peers = {1: ypos * 2 + (1 - xpos), 2: (1 - ypos) * 2 + xpos, 3: 3 - tok}
    wide = 2 * piece

    barrier = pltpu.get_barrier_semaphore()
    greet = [(tok, mate)]
    for m in (1, 2, 3):
        greet.append((peers[m], col))
        greet.append((peers[m], mate))
    for m in range(1, planes):
        greet.append((tok, ((plane + m) % planes) * 2 + core))
    for device in greet:
        pl.semaphore_signal(barrier, inc=1, device_id=device, device_id_type=MESH)
    pl.semaphore_wait(barrier, len(greet))

    def part_copy(k):
        return pltpu.make_async_remote_copy(
            src_ref=half_ref.at[1 - core, k], dst_ref=full_ref.at[k, col],
            send_sem=part_send.at[k], recv_sem=part_recv.at[k],
            device_id=(tok, mate), device_id_type=MESH)

    def part_arrival(k):
        return pltpu.make_async_remote_copy(
            src_ref=half_ref.at[1 - core, k], dst_ref=full_ref.at[k, mate],
            send_sem=part_send.at[k], recv_sem=part_recv.at[k],
            device_id=(tok, mate), device_id_type=MESH)

    def z_copy(k, j, way, own=False):
        source = half_ref.at[core, k] if own else full_ref.at[k, j]
        return pltpu.make_async_remote_copy(
            src_ref=source, dst_ref=full_ref.at[k, j],
            send_sem=z_send.at[k, j, way], recv_sem=z_recv.at[k, j],
            device_id=(tok, col + 2 - 4 * way), device_id_type=MESH)

    can = {0: plane < planes - 1, 1: plane > 0}

    def own_sends(k):
        for way in (0, 1):
            @pl.when(can[way])
            def _():
                z_copy(k, col, way, own=True).start()
        part_arrival(k).wait_recv()
        for way in (0, 1):
            @pl.when(can[way])
            def _():
                z_copy(k, mate, way).start()

    def row_copy(k, m):
        return pltpu.make_async_remote_copy(
            src_ref=rot.at[k, pl.ds(peers[m] * wide, wide)],
            dst_ref=rxr.at[k, :, pl.ds(m * rows, rows)],
            send_sem=r_send.at[k, m], recv_sem=r_recv.at[k, m],
            device_id=(peers[m], col), device_id_type=MESH)

    def col_copy(k, m):
        return pltpu.make_async_remote_copy(
            src_ref=rot.at[k, pl.ds(plane * wide, wide)],
            dst_ref=rxq.at[k, :, pl.ds(m * rows, rows)],
            send_sem=q_send.at[k, m], recv_sem=q_recv.at[k, m],
            device_id=(peers[m], col), device_id_type=MESH)

    def relay_copy(k):
        odd = k % 2
        target = peers[2] * (1 - odd) + peers[1] * odd
        start = pl.multiple_of((1 + odd) * rows, rows)
        return pltpu.make_async_remote_copy(
            src_ref=rxq.at[k, :, pl.ds(start, rows)],
            dst_ref=rxq.at[k, :, pl.ds(3 * rows, rows)],
            send_sem=q_send.at[k, 3], recv_sem=q_recv.at[k, 3],
            device_id=(target, col), device_id_type=MESH)

    def z_stage(k):
        for distance in range(1, planes):
            for way, origin in ((0, plane - distance), (1, plane + distance)):
                @pl.when((origin >= 0) & (origin < planes))
                def _():
                    for side in (0, 1):
                        j = origin * 2 + (core if side == 0 else 1 - core)
                        z_copy(k, j, way).wait_recv()

                        @pl.when(can[way])
                        def _():
                            z_copy(k, j, way).start()
            if distance == max(planes - 2, 1):
                @pl.when(k + 1 < chunks)
                def _():
                    own_sends(k + 1)

    def load_chunk(k):
        copies = [pltpu.make_async_copy(half_ref.at[core, k], xbuf.at[col], load_sem.at[0])]
        copies.append(pltpu.make_async_copy(full_ref.at[k, mate], xbuf.at[mate], load_sem.at[1]))
        for m in range(1, planes):
            other = ((plane + m) % planes) * 2
            copies.append(pltpu.make_async_copy(
                full_ref.at[k, pl.ds(other, 2)], xbuf.at[pl.ds(other, 2)], load_sem.at[1 + m]))
        for copy in copies:
            copy.start()
        for copy in copies:
            copy.wait()

    groups = 2 * planes * piece

    def rotate(k):
        def product(j, carry):
            block = xbuf[j].reshape(piece * rows, LANES)
            out = jnp.dot(block, table_ref[...], preferred_element_type=jnp.float32)
            tmp[pl.ds(j * piece, piece)] = out.reshape(piece, rows, LANES)
            return carry

        lax.fori_loop(0, 2 * planes, product, 0)

        def butterfly(index, carry):
            r = pl.multiple_of((index // (LANES // 128)) * 16, 16)
            lane = pl.multiple_of((index % (LANES // 128)) * 128, 128)
            values = [tmp[g, pl.ds(r, 16), pl.ds(lane, 128)] for g in range(groups)]
            step = 1
            while step < groups:
                values = [
                    values[g] + values[g + step] if g & step == 0 else values[g - step] - values[g]
                    for g in range(groups)
                ]
                step *= 2
            total = squares[0]
            for g in range(groups):
                rounded = (values[g] * scale).astype(jnp.bfloat16)
                rot[k, g, pl.ds(r, 16), pl.ds(lane, 128)] = rounded
                exact = rounded.astype(jnp.float32)
                total = total + exact * exact
            squares[0] = total
            return carry

        lax.fori_loop(0, (rows // 16) * (LANES // 128), butterfly, 0)
        for f in range(wide):
            rxr[k, f, pl.ds(0, rows)] = rot[k, tok * wide + f]
            rxq[k, f, pl.ds(0, rows)] = rot[k, plane * wide + f]
        for m in (1, 2):
            col_copy(k, m).start()
        for m in (1, 2, 3):
            row_copy(k, m).start()

    def arrivals(k):
        odd = k % 2

        @pl.when(odd == 0)
        def _():
            col_copy(k, 1).wait_recv()
            relay_copy(k).start()
            col_copy(k, 2).wait_recv()

        @pl.when(odd == 1)
        def _():
            col_copy(k, 2).wait_recv()
            relay_copy(k).start()
            col_copy(k, 1).wait_recv()

        for m in (1, 2, 3):
            row_copy(k, m).wait_recv()
        relay_copy(k).wait_recv()

    def row_block(k, f):
        left = rxr[k, f].T
        start = pl.multiple_of(f * LANES, LANES)
        for n in range(wide):
            out = jnp.dot(left, rxq[k, n], preferred_element_type=jnp.float32)
            acc[n // piece, pl.ds(start, LANES), pl.ds((n % piece) * LANES, LANES)] += out

    def gram(k):
        def body(f, carry):
            row_block(k, f)
            return carry

        lax.fori_loop(0, wide, body, 0)

    def gram_out(f):
        span = pl.ds(pl.multiple_of(f * LANES, LANES), LANES)
        return pltpu.make_async_remote_copy(
            src_ref=acc.at[1 - core, span], dst_ref=gram_in_ref.at[span],
            send_sem=g_send.at[f], recv_sem=g_recv.at[f],
            device_id=(tok, mate), device_id_type=MESH)

    def gram_keep(f):
        span = pl.ds(pl.multiple_of(f * LANES, LANES), LANES)
        return pltpu.make_async_copy(acc.at[core, span], gram_ref.at[span], out_sem.at[f])

    def square_copy(m):
        target = (tok, mate) if m == 4 else (peers[m % 4], col if m < 4 else mate)
        return pltpu.make_async_remote_copy(
            src_ref=squares.at[0], dst_ref=squares.at[m],
            send_sem=s_send.at[m], recv_sem=s_recv.at[m],
            device_id=target, device_id_type=MESH)

    def send_part(k, carry):
        part_copy(k).start()
        return carry

    lax.fori_loop(0, chunks, send_part, 0)
    own_sends(0)
    squares[0] = jnp.zeros((16, 128), jnp.float32)

    def clear(index, carry):
        start = pl.multiple_of((index % (acc.shape[1] // 64)) * 64, 64)
        acc[index // (acc.shape[1] // 64), pl.ds(start, 64)] = jnp.zeros((64, acc.shape[2]), jnp.float32)
        return carry

    lax.fori_loop(0, acc.shape[0] * (acc.shape[1] // 64), clear, 0)

    def step(k, carry):
        z_stage(k)
        load_chunk(k)
        rotate(k)

        @pl.when(k > 0)
        def _():
            arrivals(k - 1)
            gram(k - 1)

        return carry

    lax.fori_loop(0, chunks, step, 0)
    for m in range(1, 8):
        square_copy(m).start()
    last = chunks - 1
    arrivals(last)

    def final(f, carry):
        row_block(last, f)

        @pl.when(f > 0)
        def _():
            gram_out(f - 1).start()
            gram_keep(f - 1).start()

        return carry

    lax.fori_loop(0, wide, final, 0)
    for m in range(1, 8):
        square_copy(m).wait()
    sums = squares[0]
    for m in range(1, 8):
        sums = sums + squares[m]
    square_ref[...] = sums
    gram_out(wide - 1).start()
    gram_keep(wide - 1).start()

    def drain(k, carry):
        part_copy(k).wait_send()
        for j in range(2 * planes):
            @pl.when(can[0] & (j // 2 <= plane))
            def _():
                z_copy(k, j, 0).wait_send()

            @pl.when(can[1] & (j // 2 >= plane))
            def _():
                z_copy(k, j, 1).wait_send()
        for m in (1, 2):
            col_copy(k, m).wait_send()
        relay_copy(k).wait_send()
        for m in (1, 2, 3):
            row_copy(k, m).wait_send()
        return carry

    lax.fori_loop(0, chunks, drain, 0)

    def finish(f, carry):
        gram_out(f).wait()
        gram_keep(f).wait()
        return carry

    lax.fori_loop(0, wide, finish, 0)


def fits(row_bank, token_ids):
    col_width, tok_rows = row_bank.shape[1], token_ids.shape[0]
    col_count, tok_count = lax.axis_size("col"), lax.axis_size("tok")
    return (
        col_width % LANES == 0
        and tok_count == 4
        and col_count % 2 == 0
        and D // tok_count == 2 * col_width
        and tok_rows % 256 == 0
        and tok_rows * D * 6 + (D // tok_count) ** 2 * 4 <= 96 * 2**20
    )


def fused(row_bank, token_ids, sign_flips, damping):
    col_width = row_bank.shape[1]
    col_count = lax.axis_size("col")
    tok_count = lax.axis_size("tok")
    tok_rows = token_ids.shape[0]
    planes = col_count // 2
    own_rows = tok_rows // 2
    rows = 64
    chunks = own_rows // rows
    piece = col_width // LANES
    wide = 2 * piece
    groups = D // LANES
    spread = LANES // BLOCK
    inner = jnp.kron(jnp.eye(spread, dtype=jnp.bfloat16), hadamard(BLOCK))
    outer = jnp.kron(hadamard(spread), jnp.eye(BLOCK, dtype=jnp.bfloat16))
    picked = jnp.take(row_bank, token_ids, axis=0) * sign_flips.astype(jnp.bfloat16)[None, :]
    parts = []
    for g in range(piece):
        part = picked[:, g * LANES : (g + 1) * LANES]
        part = jnp.dot(part, inner, preferred_element_type=jnp.float32).astype(jnp.bfloat16)
        parts.append(part.reshape(2, chunks, rows, LANES))
    half = jnp.stack(parts, axis=2)
    any_space = pl.BlockSpec(memory_space=pl.ANY)
    vmem = pl.BlockSpec(memory_space=pltpu.VMEM)
    dma = pltpu.SemaphoreType.DMA
    height = D // tok_count
    gram, gram_in, squares, _ = pl.pallas_call(
        functools.partial(fused_kernel, planes, chunks, rows, piece, 1.0 / math.sqrt(D)),
        out_shape=(
            jax.ShapeDtypeStruct((height, col_width), jnp.float32),
            jax.ShapeDtypeStruct((height, col_width), jnp.float32),
            jax.ShapeDtypeStruct((16, 128), jnp.float32),
            jax.ShapeDtypeStruct((chunks, col_count, piece, rows, LANES), jnp.bfloat16),
        ),
        in_specs=[any_space, vmem],
        out_specs=(any_space, any_space, vmem, any_space),
        scratch_shapes=[
            pltpu.VMEM((col_count, piece, rows, LANES), jnp.bfloat16),
            pltpu.VMEM((groups, rows, LANES), jnp.float32),
            pltpu.VMEM((chunks, groups, rows, LANES), jnp.bfloat16),
            pltpu.VMEM((chunks, wide, 4 * rows, LANES), jnp.bfloat16),
            pltpu.VMEM((chunks, wide, 4 * rows, LANES), jnp.bfloat16),
            pltpu.VMEM((2, height, col_width), jnp.float32),
            pltpu.VMEM((8, 16, 128), jnp.float32),
            dma((chunks,)), dma((chunks,)),
            dma((chunks, col_count, 2)), dma((chunks, col_count)),
            dma((chunks, 4)), dma((chunks, 4)),
            dma((chunks, 4)), dma((chunks, 4)),
            dma((8,)), dma((8,)),
            dma((wide,)), dma((wide,)),
            dma((planes + 1,)), dma((wide,)),
        ],
        compiler_params=pltpu.CompilerParams(
            collective_id=0, has_side_effects=True, vmem_limit_bytes=67043328
        ),
    )(half, outer)
    tokens_all = tok_rows * tok_count
    mean_diag = jnp.sum(squares) / tokens_all / D
    gram_block = (gram + gram_in) / tokens_all
    return damped(gram_block, damping, mean_diag)


def damped(gram_block, damping, mean_diag):
    block_rows, col_width = gram_block.shape
    row_index = lax.axis_index("tok") * block_rows + lax.broadcasted_iota(
        jnp.int32, gram_block.shape, 0
    )
    col_index = lax.axis_index("col") * col_width + lax.broadcasted_iota(
        jnp.int32, gram_block.shape, 1
    )
    on_diag = (row_index == col_index).astype(jnp.float32)
    return gram_block + damping[0] * mean_diag * on_diag


def plain(row_bank, token_ids, sign_flips, damping):
    col_width = row_bank.shape[1]
    col_count = lax.axis_size("col")
    tok_count = lax.axis_size("tok")
    tok_rows = token_ids.shape[0]
    groups = D // BLOCK
    scale = 1.0 / math.sqrt(D)
    inner_table = hadamard(BLOCK)
    outer_table = hadamard(groups)
    col_start = lax.axis_index("col") * col_width
    picked = jnp.take(row_bank, token_ids, axis=0) * sign_flips.astype(jnp.bfloat16)[None, :]
    shaped = picked.reshape(picked.shape[0], -1, BLOCK)
    turned = jnp.einsum("rab,bc->rac", shaped, inner_table, preferred_element_type=jnp.float32)
    half_turned = turned.astype(jnp.bfloat16).reshape(picked.shape)
    grouped = half_turned.reshape(col_count, tok_rows // col_count, col_width)
    block = lax.all_to_all(grouped, "col", split_axis=0, concat_axis=2, tiled=True)[0]
    shaped = block.reshape(block.shape[0], groups, BLOCK)
    turned = (
        jnp.einsum("rab,ac->rcb", shaped, outer_table, preferred_element_type=jnp.float32) * scale
    )
    finished = turned.astype(jnp.bfloat16).reshape(block.shape)[None]
    squares = jnp.sum(jnp.square(finished.astype(jnp.float32)))
    tokens_all = tok_rows * tok_count
    square_sum = lax.psum(squares, ("tok", "col"))
    mean_diag = square_sum / tokens_all / D
    flat = lax.all_gather(finished, "col", axis=1, tiled=True).reshape(-1, D)
    own_cols = lax.dynamic_slice_in_dim(flat, col_start, col_width, 1)
    partial_sum = lax.dot_general(
        flat, own_cols, (((0,), (0,)), ((), ())), preferred_element_type=jnp.float32
    )
    gram_block = lax.psum_scatter(partial_sum, "tok", scatter_dimension=0, tiled=True) / tokens_all
    return damped(gram_block, damping, mean_diag)


def shards(row_bank, token_ids, sign_flips, damping):
    run = fused if fits(row_bank, token_ids) else plain
    return run(row_bank, token_ids, sign_flips, damping)


def solution(mesh):
    in_specs = (P(None, "col"), P("tok"), P("col"), P())
    out_specs = P("tok", "col")
    return jax.shard_map(shards, mesh=mesh, in_specs=in_specs, out_specs=out_specs, check_vma=False)
```

```python
import functools
import math

import jax
import jax.numpy as jnp
import numpy as np
from jax import lax
from jax.experimental import pallas as pl
from jax.experimental.pallas import tpu as pltpu
from jax.sharding import PartitionSpec as P

D = 8192
BLOCK = 32
LANES = 512
MESH = pl.DeviceIdType.MESH


def hadamard(order):
    index_range = jnp.arange(order, dtype=jnp.int32)
    anded = jnp.bitwise_and(index_range[:, None], index_range[None, :])
    parity = jnp.zeros((order, order), jnp.int32)
    for bit_place in range(int(order).bit_length()):
        parity = parity + jnp.bitwise_and(jnp.right_shift(anded, bit_place), 1)
    return (1 - 2 * jnp.bitwise_and(parity, 1)).astype(jnp.bfloat16)


def sylvester(order):
    table = np.ones((1, 1))
    while table.shape[0] < order:
        table = np.block([[table, table], [table, -table]])
    return table


def fused_kernel(
    planes, chunks, rows, piece, scale,
    half_ref, table_ref,
    gram_ref, gram_in_ref, square_ref, full_ref,
    xbuf, tmp, rot, rxr, rxq, acc, squares,
    part_send, part_recv, z_send, z_recv, r_send, r_recv, q_send, q_recv,
    s_send, s_recv, g_send, g_recv, load_sem, out_sem,
):
    tok = lax.axis_index("tok")
    col = lax.axis_index("col")
    plane, core = col // 2, col % 2
    mate = plane * 2 + (1 - core)
    ypos, xpos = tok // 2, tok % 2
    peers = {1: ypos * 2 + (1 - xpos), 2: (1 - ypos) * 2 + xpos, 3: 3 - tok}
    wide = 2 * piece

    barrier = pltpu.get_barrier_semaphore()
    greet = [(tok, mate)]
    for m in (1, 2, 3):
        greet.append((peers[m], col))
        greet.append((peers[m], mate))
    for m in range(1, planes):
        greet.append((tok, ((plane + m) % planes) * 2 + core))
    for device in greet:
        pl.semaphore_signal(barrier, inc=1, device_id=device, device_id_type=MESH)
    pl.semaphore_wait(barrier, len(greet))

    def part_copy(k):
        return pltpu.make_async_remote_copy(
            src_ref=half_ref.at[1 - core, k], dst_ref=full_ref.at[k, col],
            send_sem=part_send.at[k], recv_sem=part_recv.at[k],
            device_id=(tok, mate), device_id_type=MESH)

    def part_arrival(k):
        return pltpu.make_async_remote_copy(
            src_ref=half_ref.at[1 - core, k], dst_ref=full_ref.at[k, mate],
            send_sem=part_send.at[k], recv_sem=part_recv.at[k],
            device_id=(tok, mate), device_id_type=MESH)

    def z_copy(k, j, way, own=False):
        source = half_ref.at[core, k] if own else full_ref.at[k, j]
        return pltpu.make_async_remote_copy(
            src_ref=source, dst_ref=full_ref.at[k, j],
            send_sem=z_send.at[k, j, way], recv_sem=z_recv.at[k, j],
            device_id=(tok, col + 2 - 4 * way), device_id_type=MESH)

    can = {0: plane < planes - 1, 1: plane > 0}

    def own_sends(k):
        for way in (0, 1):
            @pl.when(can[way])
            def _():
                z_copy(k, col, way, own=True).start()
        part_arrival(k).wait_recv()
        for way in (0, 1):
            @pl.when(can[way])
            def _():
                z_copy(k, mate, way).start()

    def row_copy(k, m):
        return pltpu.make_async_remote_copy(
            src_ref=rot.at[k, pl.ds(peers[m] * wide, wide)],
            dst_ref=rxr.at[k, :, pl.ds(m * rows, rows)],
            send_sem=r_send.at[k, m], recv_sem=r_recv.at[k, m],
            device_id=(peers[m], col), device_id_type=MESH)

    def col_copy(k, m):
        return pltpu.make_async_remote_copy(
            src_ref=rot.at[k, pl.ds(plane * wide, wide)],
            dst_ref=rxq.at[k, :, pl.ds(m * rows, rows)],
            send_sem=q_send.at[k, m], recv_sem=q_recv.at[k, m],
            device_id=(peers[m], col), device_id_type=MESH)

    def relay_copy(k):
        odd = k % 2
        target = peers[2] * (1 - odd) + peers[1] * odd
        start = pl.multiple_of((1 + odd) * rows, rows)
        return pltpu.make_async_remote_copy(
            src_ref=rxq.at[k, :, pl.ds(start, rows)],
            dst_ref=rxq.at[k, :, pl.ds(3 * rows, rows)],
            send_sem=q_send.at[k, 3], recv_sem=q_recv.at[k, 3],
            device_id=(target, col), device_id_type=MESH)

    def z_stage(k, distance):
        for way, origin in ((0, plane - distance), (1, plane + distance)):
            @pl.when((origin >= 0) & (origin < planes))
            def _():
                for side in (0, 1):
                    j = origin * 2 + (core if side == 0 else 1 - core)
                    z_copy(k, j, way).wait_recv()

                    @pl.when(can[way])
                    def _():
                        z_copy(k, j, way).start()

    def load_chunk(k):
        copies = [pltpu.make_async_copy(half_ref.at[core, k], xbuf.at[col], load_sem.at[0])]
        copies.append(pltpu.make_async_copy(full_ref.at[k, mate], xbuf.at[mate], load_sem.at[1]))
        for m in range(1, planes):
            other = ((plane + m) % planes) * 2
            copies.append(pltpu.make_async_copy(
                full_ref.at[k, pl.ds(other, 2)], xbuf.at[pl.ds(other, 2)], load_sem.at[1 + m]))
        for copy in copies:
            copy.start()
        for copy in copies:
            copy.wait()

    groups = 2 * planes * piece

    def rotate(k):
        def product(j, carry):
            block = xbuf[j].reshape(piece * rows, LANES)
            out = jnp.dot(block, table_ref[...], preferred_element_type=jnp.float32)
            tmp[pl.ds(j * piece, piece)] = out.reshape(piece, rows, LANES)
            return carry

        lax.fori_loop(0, 2 * planes, product, 0)

        def butterfly(index, carry):
            r = pl.multiple_of((index // (LANES // 128)) * 16, 16)
            lane = pl.multiple_of((index % (LANES // 128)) * 128, 128)
            values = [tmp[g, pl.ds(r, 16), pl.ds(lane, 128)] for g in range(groups)]
            step = 1
            while step < groups:
                values = [
                    values[g] + values[g + step] if g & step == 0 else values[g - step] - values[g]
                    for g in range(groups)
                ]
                step *= 2
            total = squares[0]
            for g in range(groups):
                rounded = (values[g] * scale).astype(jnp.bfloat16)
                rot[k, g, pl.ds(r, 16), pl.ds(lane, 128)] = rounded
                exact = rounded.astype(jnp.float32)
                total = total + exact * exact
            squares[0] = total
            return carry

        lax.fori_loop(0, (rows // 16) * (LANES // 128), butterfly, 0)
        for f in range(wide):
            rxr[k, f, pl.ds(0, rows)] = rot[k, tok * wide + f]
            rxq[k, f, pl.ds(0, rows)] = rot[k, plane * wide + f]
        for m in (1, 2):
            col_copy(k, m).start()
        for m in (1, 2, 3):
            row_copy(k, m).start()

    def relay(k):
        odd = k % 2

        @pl.when(odd == 0)
        def _():
            col_copy(k, 1).wait_recv()

        @pl.when(odd == 1)
        def _():
            col_copy(k, 2).wait_recv()

        relay_copy(k).start()

    def arrivals(k):
        odd = k % 2

        @pl.when(odd == 0)
        def _():
            col_copy(k, 2).wait_recv()

        @pl.when(odd == 1)
        def _():
            col_copy(k, 1).wait_recv()

        for m in (1, 2, 3):
            row_copy(k, m).wait_recv()
        relay_copy(k).wait_recv()

    def row_block(k, f):
        left = rxr[k, f].T
        start = pl.multiple_of(f * LANES, LANES)
        for n in range(wide):
            out = jnp.dot(left, rxq[k, n], preferred_element_type=jnp.float32)
            acc[n // piece, pl.ds(start, LANES), pl.ds((n % piece) * LANES, LANES)] += out

    def gram(k):
        def body(f, carry):
            row_block(k, f)
            return carry

        lax.fori_loop(0, wide, body, 0)

    def gram_out(f):
        span = pl.ds(pl.multiple_of(f * LANES, LANES), LANES)
        return pltpu.make_async_remote_copy(
            src_ref=acc.at[1 - core, span], dst_ref=gram_in_ref.at[span],
            send_sem=g_send.at[f], recv_sem=g_recv.at[f],
            device_id=(tok, mate), device_id_type=MESH)

    def gram_keep(f):
        span = pl.ds(pl.multiple_of(f * LANES, LANES), LANES)
        return pltpu.make_async_copy(acc.at[core, span], gram_ref.at[span], out_sem.at[f])

    def square_copy(m):
        target = (tok, mate) if m == 4 else (peers[m % 4], col if m < 4 else mate)
        return pltpu.make_async_remote_copy(
            src_ref=squares.at[0], dst_ref=squares.at[m],
            send_sem=s_send.at[m], recv_sem=s_recv.at[m],
            device_id=target, device_id_type=MESH)

    def send_part(k, carry):
        part_copy(k).start()
        return carry

    lax.fori_loop(0, chunks, send_part, 0)
    own_sends(0)
    squares[0] = jnp.zeros((16, 128), jnp.float32)

    def clear(index, carry):
        start = pl.multiple_of((index % (acc.shape[1] // 64)) * 64, 64)
        acc[index // (acc.shape[1] // 64), pl.ds(start, 64)] = jnp.zeros((64, acc.shape[2]), jnp.float32)
        return carry

    lax.fori_loop(0, acc.shape[0] * (acc.shape[1] // 64), clear, 0)
    for distance in range(1, planes - 1):
        z_stage(0, distance)
    if chunks > 1:
        own_sends(1)

    def step(k, carry):
        z_stage(k, planes - 1)
        if planes > 2:
            @pl.when(k + 1 < chunks)
            def _():
                z_stage(k + 1, 1)

        @pl.when(k + 2 < chunks)
        def _():
            own_sends(k + 2)

        @pl.when(k > 0)
        def _():
            relay(k - 1)

        load_chunk(k)
        rotate(k)

        @pl.when(k + 1 < chunks)
        def _():
            for distance in range(2, planes - 1):
                z_stage(k + 1, distance)

        @pl.when(k > 1)
        def _():
            arrivals(k - 2)
            gram(k - 2)

        return carry

    lax.fori_loop(0, chunks, step, 0)
    for m in range(1, 8):
        square_copy(m).start()
    last = chunks - 1
    if chunks > 1:
        arrivals(last - 1)
        gram(last - 1)
    relay(last)
    arrivals(last)

    def final(f, carry):
        row_block(last, f)

        @pl.when(f > 0)
        def _():
            gram_out(f - 1).start()
            gram_keep(f - 1).start()

        return carry

    lax.fori_loop(0, wide, final, 0)
    for m in range(1, 8):
        square_copy(m).wait()
    sums = squares[0]
    for m in range(1, 8):
        sums = sums + squares[m]
    square_ref[...] = sums
    gram_out(wide - 1).start()
    gram_keep(wide - 1).start()

    def drain(k, carry):
        part_copy(k).wait_send()
        for j in range(2 * planes):
            @pl.when(can[0] & (j // 2 <= plane))
            def _():
                z_copy(k, j, 0).wait_send()

            @pl.when(can[1] & (j // 2 >= plane))
            def _():
                z_copy(k, j, 1).wait_send()
        for m in (1, 2):
            col_copy(k, m).wait_send()
        relay_copy(k).wait_send()
        for m in (1, 2, 3):
            row_copy(k, m).wait_send()
        return carry

    lax.fori_loop(0, chunks, drain, 0)

    def finish(f, carry):
        gram_out(f).wait()
        gram_keep(f).wait()
        return carry

    lax.fori_loop(0, wide, finish, 0)


def fits(row_bank, token_ids):
    col_width, tok_rows = row_bank.shape[1], token_ids.shape[0]
    col_count, tok_count = lax.axis_size("col"), lax.axis_size("tok")
    return (
        col_width % LANES == 0
        and tok_count == 4
        and col_count % 2 == 0
        and D // tok_count == 2 * col_width
        and tok_rows % 256 == 0
        and tok_rows * D * 6 + (D // tok_count) ** 2 * 4 <= 96 * 2**20
    )


def fused(row_bank, token_ids, sign_flips, damping):
    col_width = row_bank.shape[1]
    col_count = lax.axis_size("col")
    tok_count = lax.axis_size("tok")
    tok_rows = token_ids.shape[0]
    planes = col_count // 2
    own_rows = tok_rows // 2
    rows = 64
    chunks = own_rows // rows
    piece = col_width // LANES
    wide = 2 * piece
    groups = D // LANES
    spread = LANES // BLOCK
    inner = jnp.asarray(np.kron(np.eye(spread), sylvester(BLOCK)), jnp.bfloat16)
    outer = jnp.asarray(np.kron(sylvester(spread), np.eye(BLOCK)), jnp.bfloat16)
    signs = sign_flips.astype(jnp.bfloat16)[:, None]
    picked = jnp.take(row_bank, token_ids, axis=0)
    parts = []
    for g in range(piece):
        part = picked[:, g * LANES : (g + 1) * LANES]
        table = inner * signs[g * LANES : (g + 1) * LANES]
        part = jnp.dot(part, table, preferred_element_type=jnp.float32).astype(jnp.bfloat16)
        parts.append(part.reshape(2, chunks, rows, LANES))
    half = jnp.stack(parts, axis=2)
    any_space = pl.BlockSpec(memory_space=pl.ANY)
    vmem = pl.BlockSpec(memory_space=pltpu.VMEM)
    dma = pltpu.SemaphoreType.DMA
    height = D // tok_count
    gram, gram_in, squares, _ = pl.pallas_call(
        functools.partial(fused_kernel, planes, chunks, rows, piece, 1.0 / math.sqrt(D)),
        out_shape=(
            jax.ShapeDtypeStruct((height, col_width), jnp.float32),
            jax.ShapeDtypeStruct((height, col_width), jnp.float32),
            jax.ShapeDtypeStruct((16, 128), jnp.float32),
            jax.ShapeDtypeStruct((chunks, col_count, piece, rows, LANES), jnp.bfloat16),
        ),
        in_specs=[any_space, vmem],
        out_specs=(any_space, any_space, vmem, any_space),
        scratch_shapes=[
            pltpu.VMEM((col_count, piece, rows, LANES), jnp.bfloat16),
            pltpu.VMEM((groups, rows, LANES), jnp.float32),
            pltpu.VMEM((chunks, groups, rows, LANES), jnp.bfloat16),
            pltpu.VMEM((chunks, wide, 4 * rows, LANES), jnp.bfloat16),
            pltpu.VMEM((chunks, wide, 4 * rows, LANES), jnp.bfloat16),
            pltpu.VMEM((2, height, col_width), jnp.float32),
            pltpu.VMEM((8, 16, 128), jnp.float32),
            dma((chunks,)), dma((chunks,)),
            dma((chunks, col_count, 2)), dma((chunks, col_count)),
            dma((chunks, 4)), dma((chunks, 4)),
            dma((chunks, 4)), dma((chunks, 4)),
            dma((8,)), dma((8,)),
            dma((wide,)), dma((wide,)),
            dma((planes + 1,)), dma((wide,)),
        ],
        compiler_params=pltpu.CompilerParams(
            collective_id=0, has_side_effects=True, vmem_limit_bytes=67043328
        ),
    )(half, outer)
    tokens_all = tok_rows * tok_count
    mean_diag = jnp.sum(squares) / tokens_all / D
    gram_block = (gram + gram_in) / tokens_all
    return damped(gram_block, damping, mean_diag)


def damped(gram_block, damping, mean_diag):
    block_rows, col_width = gram_block.shape
    row_index = lax.axis_index("tok") * block_rows + lax.broadcasted_iota(
        jnp.int32, gram_block.shape, 0
    )
    col_index = lax.axis_index("col") * col_width + lax.broadcasted_iota(
        jnp.int32, gram_block.shape, 1
    )
    on_diag = (row_index == col_index).astype(jnp.float32)
    return gram_block + damping[0] * mean_diag * on_diag


def plain(row_bank, token_ids, sign_flips, damping):
    col_width = row_bank.shape[1]
    col_count = lax.axis_size("col")
    tok_count = lax.axis_size("tok")
    tok_rows = token_ids.shape[0]
    groups = D // BLOCK
    scale = 1.0 / math.sqrt(D)
    inner_table = hadamard(BLOCK)
    outer_table = hadamard(groups)
    col_start = lax.axis_index("col") * col_width
    picked = jnp.take(row_bank, token_ids, axis=0) * sign_flips.astype(jnp.bfloat16)[None, :]
    shaped = picked.reshape(picked.shape[0], -1, BLOCK)
    turned = jnp.einsum("rab,bc->rac", shaped, inner_table, preferred_element_type=jnp.float32)
    half_turned = turned.astype(jnp.bfloat16).reshape(picked.shape)
    grouped = half_turned.reshape(col_count, tok_rows // col_count, col_width)
    block = lax.all_to_all(grouped, "col", split_axis=0, concat_axis=2, tiled=True)[0]
    shaped = block.reshape(block.shape[0], groups, BLOCK)
    turned = (
        jnp.einsum("rab,ac->rcb", shaped, outer_table, preferred_element_type=jnp.float32) * scale
    )
    finished = turned.astype(jnp.bfloat16).reshape(block.shape)[None]
    squares = jnp.sum(jnp.square(finished.astype(jnp.float32)))
    tokens_all = tok_rows * tok_count
    square_sum = lax.psum(squares, ("tok", "col"))
    mean_diag = square_sum / tokens_all / D
    flat = lax.all_gather(finished, "col", axis=1, tiled=True).reshape(-1, D)
    own_cols = lax.dynamic_slice_in_dim(flat, col_start, col_width, 1)
    partial_sum = lax.dot_general(
        flat, own_cols, (((0,), (0,)), ((), ())), preferred_element_type=jnp.float32
    )
    gram_block = lax.psum_scatter(partial_sum, "tok", scatter_dimension=0, tiled=True) / tokens_all
    return damped(gram_block, damping, mean_diag)


def shards(row_bank, token_ids, sign_flips, damping):
    run = fused if fits(row_bank, token_ids) else plain
    return run(row_bank, token_ids, sign_flips, damping)


def solution(mesh):
    in_specs = (P(None, "col"), P("tok"), P("col"), P())
    out_specs = P("tok", "col")
    return jax.shard_map(shards, mesh=mesh, in_specs=in_specs, out_specs=out_specs, check_vma=False)
```
